32 devices in a mesh: img: 4 (over y, core), proj: 8 (over z, x).
Axes of the slice: x: 2, y: 2, z: 4, core: 2. Of those that a mesh axis runs over, the one named last changes fastest.
Arguments:
- images: bfloat16 [512, 4096], P('img'), may hold values from -48 to 48
- projections: bfloat16 [2560, 4096], P('proj'), may hold values from -6 to 6
- noise_weight: float32 [4096], replicated, may hold values from 0.02 to 0.08
- defocus: float32 [512], P('img'), may hold values from 2 to 8
- orient_count: int32 [512], P('img'), may hold values from 160 to 2560, as said below
- term_limit: int32 [512], P('img'), may hold values from 2048 to 4096
- block_plan: int32 [16], replicated, may hold values from 0 to 15, each once
Outputs:
- reconstruction: bfloat16 [2560, 4096], P('proj', 'img')
- evidence_next: float32 [512], P('img')
The draws below stay inside these ranges and needn't reach their ends.
Inputs may be any that keep to these rules, and one draw needn't show every extreme that they name: Orientations 0 to orient_count[i] - 1 are the significant ones of image i; some image has all 2560.
All inputs are finite; a program needn't handle non-finite values.
Results may differ from the reference program's by a relative error of at most 0.018.
Values may be sent and summed in bfloat16 or wider, within the bound.
A program may use at most 64 MiB of HBM per device.

```python
import math
import jax
import jax.numpy as jnp
from jax import lax

F = 4096
NPROJ = 2560
IMG_DEV = 128
BLOCK = 32
NIMG = 512
NBLK = 16
N_IMG = 4


def shared_draw(key):
    projections = jnp.clip(jax.random.normal(jax.random.fold_in(key, 101), (NPROJ, F), jnp.float32), -6.0, 6.0)
    defocus = jax.random.uniform(jax.random.fold_in(key, 102), (NIMG,), jnp.float32, 2.0, 8.0)
    pixels = jnp.clip(jax.random.normal(jax.random.fold_in(key, 103), (NIMG, F), jnp.float32), -6.0, 6.0)
    return (projections, defocus, pixels)


def draw_projections(key, part):
    return shared_draw(key)[0].astype(jnp.bfloat16)


def draw_defocus(key, part):
    return shared_draw(key)[1]


def draw_images(key, part):
    projections, defocus, pixels = shared_draw(key)
    row_ids = jnp.arange(NIMG, dtype=jnp.int32)
    chosen = row_ids % 16 == 5
    first_pick = jax.random.randint(jax.random.fold_in(key, 105), (NIMG,), 0, max(NPROJ // 16 - 1, 1))
    second_pick = first_pick + 1
    strength = jnp.array([2.0, 3.0, 4.0], jnp.float32)[row_ids // 16 % 3]
    frequency = (jnp.arange(F, dtype=jnp.float32) + 1.0) / F
    contrast = jnp.sin(2.0 * math.pi * defocus[:, None] * frequency[None, :] + 0.1)
    aligned = strength[:, None] * contrast * (projections[first_pick] + projections[second_pick])
    pixels = jnp.where(chosen[:, None], aligned, pixels)
    return pixels.astype(jnp.bfloat16)


def draw_orient_count(key, part):
    lowest = NPROJ // 16
    level = jax.random.randint(jax.random.fold_in(key, 201), (NIMG // IMG_DEV,), lowest, NPROJ + 1)
    level = jnp.repeat(level, IMG_DEV)
    spread = jax.random.randint(jax.random.fold_in(key, 202), (NIMG,), 0, 1 << 20)
    counts = lowest + spread % (level - lowest + 1)
    return counts.at[0].set(NPROJ).astype(jnp.int32)


def place_ends(values, stream_key, smallest, high):
    shape = values.shape
    place = [jax.random.randint(jax.random.fold_in(stream_key, axis), (), 0, shape[axis]) for axis in range(len(shape))]
    values = values.at[tuple(place)].set(smallest)
    longest = shape.index(max(shape))
    place[longest] = (place[longest] + 1) % shape[longest]
    return values.at[tuple(place)].set(high)


def setup_inputs(seed: int = 0) -> dict:
    streams_of = jax.random.split(jax.random.key(seed), 8)
    return {
        "images": draw_images(jax.random.fold_in(streams_of[7], 71), 0),
        "projections": draw_projections(jax.random.fold_in(streams_of[7], 71), 0),
        "noise_weight": jnp.clip(jnp.exp(jax.random.uniform(streams_of[2], (F,), jnp.float32, math.log(0.02), math.log(0.08))), 0.02, 0.08),
        "defocus": draw_defocus(jax.random.fold_in(streams_of[7], 71), 0),
        "orient_count": draw_orient_count(jax.random.fold_in(streams_of[7], 71), 0),
        "term_limit": place_ends(jax.random.randint(streams_of[5], (NIMG,), F // 2, F + 1), jax.random.fold_in(streams_of[5], 1), F // 2, F).astype(jnp.int32),
        "block_plan": jax.random.permutation(streams_of[6], NBLK).astype(jnp.int32),
    }


def contrast_table(defocus, width):
    frequency = (jnp.arange(width, dtype=jnp.float32) + 1.0) / width
    return jnp.sin(2.0 * math.pi * defocus[:, None] * frequency[None, :] + 0.1)


def image_terms(pixels, noise_weight, defocus, limits):
    width = pixels.shape[1]
    contrast = contrast_table(defocus, width)
    keep_mask = (jnp.arange(width, dtype=jnp.int32)[None, :] < limits[:, None]).astype(contrast.dtype)
    values = pixels.astype(contrast.dtype)
    weighted = (keep_mask * noise_weight[None, :] * contrast * values).astype(jnp.bfloat16)
    weighted_sq = (keep_mask * noise_weight[None, :] * contrast * contrast).astype(jnp.bfloat16)
    back_images = (keep_mask * contrast * values).astype(jnp.bfloat16)
    back_weights = (keep_mask * contrast * contrast).astype(jnp.bfloat16)
    return weighted, weighted_sq, back_images, back_weights


def reference(images, projections, noise_weight, defocus, orient_count, term_limit, block_plan):
    wide = projections.astype(jnp.float32)
    proj_sq = (wide * wide).astype(jnp.bfloat16)
    orient_ids = jnp.arange(NPROJ, dtype=jnp.int32)

    def one_block(totals, segment):
        pixels, focus, counts, limits = segment
        weighted, weighted_sq, back_images, back_weights = image_terms(pixels, noise_weight, focus, limits)
        scores = jnp.dot(projections, weighted.T, preferred_element_type=jnp.float32)
        scores = scores - 0.5 * jnp.dot(proj_sq, weighted_sq.T, preferred_element_type=jnp.float32)
        significant = orient_ids[:, None] < counts[None, :]
        row_peak = jnp.max(jnp.where(significant, scores, -1e30), axis=0)
        safe = jnp.where(significant, scores, row_peak[None, :])
        row_mass = jnp.sum(jnp.where(significant, jnp.exp(safe - row_peak[None, :]), 0.0), axis=0)
        log_evidence = row_peak + jnp.log(row_mass)
        posterior = jnp.where(significant, jnp.exp(safe - log_evidence[None, :]), 0.0).astype(jnp.bfloat16)
        part_images = jnp.dot(posterior, back_images, preferred_element_type=jnp.float32).astype(jnp.bfloat16)
        part_weights = jnp.dot(posterior, back_weights, preferred_element_type=jnp.float32).astype(jnp.bfloat16)
        part_images = lax.optimization_barrier(part_images).astype(totals[0].dtype)
        part_weights = lax.optimization_barrier(part_weights).astype(totals[1].dtype)
        return (totals[0] + part_images, totals[1] + part_weights), log_evidence

    segments = (images.reshape(N_IMG, IMG_DEV, F), defocus.reshape(N_IMG, IMG_DEV),
                orient_count.reshape(N_IMG, IMG_DEV), term_limit.reshape(N_IMG, IMG_DEV))
    empty_sum = jnp.zeros((NPROJ, F), jnp.float32)
    (sum_images, sum_weights), evidence = lax.scan(one_block, (empty_sum, empty_sum), segments)
    reconstruction = (sum_images / (sum_weights + 1.0)).astype(jnp.bfloat16)
    evidence = evidence.reshape(NBLK, BLOCK)
    placed = jnp.zeros_like(evidence).at[block_plan].set(evidence)
    return reconstruction, placed.reshape(NIMG)
```

```python
import functools
import math

import jax
import jax.numpy as jnp
from jax import lax
from jax.experimental import pallas as pl
from jax.experimental.pallas import tpu as pltpu
from jax.sharding import PartitionSpec as P

BLOCK = 32
LANES = 128
MESH = pl.DeviceIdType.MESH
SIN_TERMS = [(-1.0) ** k * math.pi ** (2 * k + 1) / math.factorial(2 * k + 1) for k in range(7)]
COS_TERMS = [(-1.0) ** k * math.pi ** (2 * k) / math.factorial(2 * k) for k in range(8)]


def horner(terms, x):
    total = jnp.full_like(x, terms[-1])
    for term in terms[-2::-1]:
        total = total * x + term
    return total


def sincos_turns(turns):
    rest = turns - jnp.floor(turns + 0.5)
    square = rest * rest
    half_sin = rest * horner(SIN_TERMS, square)
    half_cos = horner(COS_TERMS, square)
    return 2.0 * half_sin * half_cos, 1.0 - 2.0 * half_sin * half_sin


def columns_of(row, rows):
    return jnp.broadcast_to(row, (LANES, rows)).T


def kernel(n_img, n_proj, img_hbm, proj_hbm, noise_ref, focus_ref, count_ref, limit_ref, plan_ref,
           rec_ref, ev_ref,
           img, proj, weighted, weighted_sq, moved, contrast, back_img, back_wgt, every_post,
           focus_all, limit_all, terms, every_terms, stats, every_stats, scale_out, every_scale,
           load_sem, small_send, small_recv, img_send, img_recv, post_send, post_recv,
           stat_send, stat_recv, scale_send, scale_recv):
    me = lax.axis_index("img")
    mine = lax.axis_index("proj")
    img_rows, width = img.shape
    proj_rows = proj.shape[0]
    part = width // n_img
    img_peers = [lax.rem(me + k, n_img) for k in range(1, n_img)]
    img_from = [lax.rem(me + n_img - k, n_img) for k in range(1, n_img)]
    proj_peers = [lax.rem(mine + k, n_proj) for k in range(1, n_proj)]

    barrier = pltpu.get_barrier_semaphore()
    for peer in img_peers:
        pl.semaphore_signal(barrier, inc=1, device_id={"img": peer}, device_id_type=MESH)
    for peer in proj_peers:
        pl.semaphore_signal(barrier, inc=1, device_id={"proj": peer}, device_id_type=MESH)
    load_img = pltpu.make_async_copy(img_hbm, img, load_sem.at[0])
    load_proj = pltpu.make_async_copy(proj_hbm, proj, load_sem.at[1])
    load_img.start()
    load_proj.start()

    lane = lax.broadcasted_iota(jnp.int32, (1, LANES), 1).astype(jnp.float32)
    phase = 0.1 / (2.0 * math.pi)
    focus = columns_of(focus_ref[...], img_rows)
    limit = columns_of(limit_ref[...].astype(jnp.float32), img_rows)
    sin0, cos0 = sincos_turns(focus * ((lane + 1.0) / width) + phase)
    sin_d, cos_d = sincos_turns(focus * (LANES / width))

    load_img.wait()
    pl.semaphore_wait(barrier, n_img + n_proj - 2)

    small = []
    moves = []
    for k, peer in enumerate(img_peers):
        for t, (ref, dst) in enumerate(((focus_ref, focus_all), (limit_ref, limit_all))):
            small.append(pltpu.make_async_remote_copy(
                src_ref=ref, dst_ref=dst.at[me], send_sem=small_send.at[t, k],
                recv_sem=small_recv.at[t, k], device_id={"img": peer}, device_id_type=MESH))
    for k, peer in enumerate(img_peers):
        moves.append(pltpu.make_async_remote_copy(
            src_ref=img.at[:, pl.ds(pl.multiple_of(peer * part, LANES), part)],
            dst_ref=moved.at[me], send_sem=img_send.at[k], recv_sem=img_recv.at[k],
            device_id={"img": peer}, device_id_type=MESH))
    for copy in small + moves:
        copy.start()

    def terms_chunk(c, carry):
        sin_v, cos_v = carry
        cols = pl.ds(pl.multiple_of(c * LANES, LANES), LANES)
        term = lane + (c * LANES).astype(jnp.float32)
        kept = jnp.where(term < limit, sin_v, 0.0)
        noisy = kept * noise_ref[:, cols]
        weighted[:, cols] = (noisy * img[:, cols].astype(jnp.float32)).astype(jnp.bfloat16)
        weighted_sq[:, cols] = (noisy * (-0.5 * sin_v)).astype(jnp.bfloat16)
        return sin_v * cos_d + cos_v * sin_d, cos_v * cos_d - sin_v * sin_d

    lax.fori_loop(0, width // LANES, terms_chunk, (sin0, cos0), unroll=2)
    load_proj.wait()

    depth = 512
    contract = (((1,), (1,)), ((), ()))

    def score_chunk(c, total):
        cols = pl.ds(pl.multiple_of(c * depth, depth), depth)
        rows = proj[:, cols]
        total = total + lax.dot_general(rows, weighted[:, cols], contract, preferred_element_type=jnp.float32)
        return total + lax.dot_general(rows * rows, weighted_sq[:, cols], contract,
                                       preferred_element_type=jnp.float32)

    scores = lax.fori_loop(0, width // depth, score_chunk, jnp.zeros((proj_rows, img_rows), jnp.float32))

    orient = lax.broadcasted_iota(jnp.int32, (proj_rows, img_rows), 0) + mine * proj_rows
    significant = orient < count_ref[...]
    peak = jnp.max(jnp.where(significant, scores, -1e30), axis=0, keepdims=True)
    expo = jnp.where(significant, jnp.exp(jnp.where(significant, scores - peak, 0.0)), 0.0)
    mass = jnp.sum(expo, axis=0, keepdims=True)
    stats[0:1, :] = peak
    stats[1:2, :] = mass
    terms[...] = expo.astype(jnp.bfloat16)

    stat_copies = []
    for k, peer in enumerate(proj_peers):
        stat_copies.append(pltpu.make_async_remote_copy(
            src_ref=stats, dst_ref=every_stats.at[mine], send_sem=stat_send.at[k],
            recv_sem=stat_recv.at[k], device_id={"proj": peer}, device_id_type=MESH))
        stat_copies[-1].start()
    post_copies = []
    for k, peer in enumerate(img_peers):
        post_copies.append(pltpu.make_async_remote_copy(
            src_ref=terms, dst_ref=every_terms.at[me], send_sem=post_send.at[k],
            recv_sem=post_recv.at[k], device_id={"img": peer}, device_id_type=MESH))
        post_copies[-1].start()

    for copy in small:
        copy.wait()
    focus_all[me] = focus_ref[...]
    limit_all[me] = limit_ref[...]
    start = (me * part).astype(jnp.float32)
    term0 = lane + start

    def weights_block(b, carry):
        focus_b = columns_of(focus_all[b], img_rows)
        limit_b = columns_of(limit_all[b].astype(jnp.float32), img_rows)
        sin_v, cos_v = sincos_turns(focus_b * ((term0 + 1.0) / width) + phase)
        sin_b, cos_b = sincos_turns(focus_b * (LANES / width))
        rows = pl.ds(pl.multiple_of(b * img_rows, img_rows), img_rows)
        for c in range(part // LANES):
            cols = slice(c * LANES, (c + 1) * LANES)
            kept = jnp.where(term0 + float(c * LANES) < limit_b, sin_v, 0.0)
            contrast[rows, cols] = kept
            back_wgt[rows, cols] = (kept * sin_v).astype(jnp.bfloat16)
            sin_v, cos_v = sin_v * cos_b + cos_v * sin_b, cos_v * cos_b - sin_v * sin_b
        return carry

    lax.fori_loop(0, n_img, weights_block, 0)

    every_stats[mine] = stats[...]
    for copy in stat_copies:
        copy.wait()
    peaks = [every_stats[q, 0:1, :] for q in range(n_proj)]
    top = functools.reduce(jnp.maximum, peaks)
    whole = sum(every_stats[q, 1:2, :] * jnp.exp(peaks[q] - top) for q in range(n_proj))
    evidence = top + jnp.log(whole)
    scale_out[0:1, :] = jnp.exp(peak - evidence)
    scale_out[1:2, :] = evidence
    scale_copies = []
    for k, peer in enumerate(img_peers):
        scale_copies.append(pltpu.make_async_remote_copy(
            src_ref=scale_out, dst_ref=every_scale.at[me], send_sem=scale_send.at[k],
            recv_sem=scale_recv.at[k], device_id={"img": peer}, device_id_type=MESH))
        scale_copies[-1].start()
    every_scale[me] = scale_out[...]

    def take_images(b, pixels):
        rows = pl.ds(pl.multiple_of(b * img_rows, img_rows), img_rows)
        back_img[rows, :] = (contrast[rows, :] * pixels.astype(jnp.float32)).astype(jnp.bfloat16)

    def take_post(b, values):
        cols = pl.ds(pl.multiple_of(b * img_rows, img_rows), img_rows)
        every_post[:, cols] = (values.astype(jnp.float32) * every_scale[b][0:1, :]).astype(jnp.bfloat16)

    take_images(me, img[:, pl.ds(pl.multiple_of(me * part, LANES), part)])
    every_post[:, pl.ds(pl.multiple_of(me * img_rows, img_rows), img_rows)] = (
        expo * every_scale[me][0:1, :]).astype(jnp.bfloat16)
    for k, source in enumerate(img_from):
        moves[k].wait()
        take_images(source, moved[source])
    for k, source in enumerate(img_from):
        post_copies[k].wait()
        scale_copies[k].wait()
        take_post(source, every_terms[source])

    step = min(part, 256)
    posts = every_post[...]
    for c in range(part // step):
        cols = slice(c * step, (c + 1) * step)
        sums = jnp.dot(posts, back_img[:, cols], preferred_element_type=jnp.float32)
        weights = jnp.dot(posts, back_wgt[:, cols], preferred_element_type=jnp.float32)
        rec_ref[:, cols] = (sums / (weights + 1.0)).astype(jnp.bfloat16)

    groups = img_rows // BLOCK
    group = lax.broadcasted_iota(jnp.int32, (1, img_rows), 1) // BLOCK
    placed = jnp.zeros((1, img_rows), jnp.float32)
    for a in range(n_img):
        plan = jnp.zeros((1, img_rows), jnp.int32)
        for g in range(groups):
            plan = jnp.where(group == g, plan_ref[a * groups + g], plan)
        values = every_scale[a][1:2, :]
        for t in range(groups):
            turned, target = values, plan
            if t:
                turned = pltpu.roll(values, t * BLOCK, 1)
                target = pltpu.roll(plan, t * BLOCK, 1)
            placed = placed + jnp.where(target == me * groups + group, turned, 0.0)
    ev_ref[...] = placed


def shards(n_img, n_proj, images, projections, noise_weight, defocus, orient_count, term_limit, block_plan):
    img_rows, width = images.shape
    proj_rows = projections.shape[0]
    part = width // n_img
    vmem = pl.BlockSpec(memory_space=pltpu.VMEM)
    hbm = pl.BlockSpec(memory_space=pl.ANY)
    smem = pl.BlockSpec(memory_space=pltpu.SMEM)
    bf16, f32 = jnp.bfloat16, jnp.float32
    dma = pltpu.SemaphoreType.DMA
    reconstruction, evidence = pl.pallas_call(
        functools.partial(kernel, n_img, n_proj),
        out_shape=(jax.ShapeDtypeStruct((proj_rows, part), bf16), jax.ShapeDtypeStruct((1, img_rows), f32)),
        in_specs=[hbm, hbm, vmem, vmem, vmem, vmem, smem],
        out_specs=(vmem, vmem),
        scratch_shapes=[
            pltpu.VMEM((img_rows, width), bf16),
            pltpu.VMEM((proj_rows, width), bf16),
            pltpu.VMEM((img_rows, width), bf16),
            pltpu.VMEM((img_rows, width), bf16),
            pltpu.VMEM((n_img, img_rows, part), bf16),
            pltpu.VMEM((n_img * img_rows, part), f32),
            pltpu.VMEM((n_img * img_rows, part), bf16),
            pltpu.VMEM((n_img * img_rows, part), bf16),
            pltpu.VMEM((proj_rows, n_img * img_rows), bf16),
            pltpu.VMEM((n_img, 1, img_rows), f32),
            pltpu.VMEM((n_img, 1, img_rows), jnp.int32),
            pltpu.VMEM((proj_rows, img_rows), bf16),
            pltpu.VMEM((n_img, proj_rows, img_rows), bf16),
            pltpu.VMEM((2, img_rows), f32),
            pltpu.VMEM((n_proj, 2, img_rows), f32),
            pltpu.VMEM((2, img_rows), f32),
            pltpu.VMEM((n_img, 2, img_rows), f32),
            dma((2,)),
            dma((2, n_img)), dma((2, n_img)),
            dma((n_img,)), dma((n_img,)),
            dma((n_img,)), dma((n_img,)),
            dma((n_proj,)), dma((n_proj,)),
            dma((n_img,)), dma((n_img,)),
        ],
        compiler_params=pltpu.CompilerParams(
            collective_id=0, has_side_effects=True, vmem_limit_bytes=40 * 1024 * 1024),
    )(images, projections, noise_weight.reshape(1, -1), defocus.reshape(1, -1), orient_count.reshape(1, -1),
      term_limit.reshape(1, -1), block_plan)
    return reconstruction, evidence.reshape(-1)


def solution(mesh):
    n_img, n_proj = mesh.shape["img"], mesh.shape["proj"]
    placed = (P("img", None), P("proj", None), P(), P("img"), P("img"), P("img"), P())
    return jax.shard_map(
        functools.partial(shards, n_img, n_proj), mesh=mesh, in_specs=placed,
        out_specs=(P("proj", "img"), P("img")), check_vma=False,
    )
```

```python
import functools
import math

import jax
import jax.numpy as jnp
from jax import lax
from jax.experimental import pallas as pl
from jax.experimental.pallas import tpu as pltpu
from jax.sharding import PartitionSpec as P

BLOCK = 32
LANES = 128
MESH = pl.DeviceIdType.MESH
SIN_TERMS = [(-1.0) ** k * math.pi ** (2 * k + 1) / math.factorial(2 * k + 1) for k in range(7)]
COS_TERMS = [(-1.0) ** k * math.pi ** (2 * k) / math.factorial(2 * k) for k in range(8)]


def horner(terms, x):
    total = jnp.full_like(x, terms[-1])
    for term in terms[-2::-1]:
        total = total * x + term
    return total


def sincos_turns(turns):
    rest = turns - jnp.floor(turns + 0.5)
    square = rest * rest
    half_sin = rest * horner(SIN_TERMS, square)
    half_cos = horner(COS_TERMS, square)
    return 2.0 * half_sin * half_cos, 1.0 - 2.0 * half_sin * half_sin


def columns_of(row, rows):
    return jnp.broadcast_to(row, (LANES, rows)).T


def kernel(n_img, n_proj, img_hbm, proj_hbm, noise_hbm, focus_hbm, count_hbm, limit_hbm, plan_hbm,
           rec_ref, ev_ref,
           img, proj, noise_ref, focus_ref, count_ref, limit_ref, plan_ref, weighted, weighted_sq, moved, contrast, back_img, back_wgt, every_post,
           focus_all, limit_all, terms, every_terms, stats, every_stats, scale_out, every_scale,
           load_sem, small_send, small_recv, img_send, img_recv, post_send, post_recv,
           stat_send, stat_recv, scale_send, scale_recv):
    me = lax.axis_index("img")
    mine = lax.axis_index("proj")
    img_rows, width = img.shape
    proj_rows = proj.shape[0]
    part = width // n_img
    img_peers = [lax.rem(me + k, n_img) for k in range(1, n_img)]
    img_from = [lax.rem(me + n_img - k, n_img) for k in range(1, n_img)]
    proj_peers = [lax.rem(mine + k, n_proj) for k in range(1, n_proj)]

    barrier = pltpu.get_barrier_semaphore()
    for peer in img_peers:
        pl.semaphore_signal(barrier, inc=1, device_id={"img": peer}, device_id_type=MESH)
    for peer in proj_peers:
        pl.semaphore_signal(barrier, inc=1, device_id={"proj": peer}, device_id_type=MESH)
    sources = (focus_hbm, limit_hbm, img_hbm, noise_hbm, count_hbm, plan_hbm, proj_hbm)
    targets = (focus_ref, limit_ref, img, noise_ref, count_ref, plan_ref, proj)
    loads = [pltpu.make_async_copy(source, target, load_sem.at[n])
             for n, (source, target) in enumerate(zip(sources, targets))]
    for load in loads:
        load.start()
    loads[0].wait()
    loads[1].wait()

    lane = lax.broadcasted_iota(jnp.int32, (1, LANES), 1).astype(jnp.float32)
    phase = 0.1 / (2.0 * math.pi)
    focus = columns_of(focus_ref[...], img_rows)
    limit = columns_of(limit_ref[...].astype(jnp.float32), img_rows)
    sin0, cos0 = sincos_turns(focus * ((lane + 1.0) / width) + phase)
    sin_d, cos_d = sincos_turns(focus * (LANES / width))

    for load in loads[2:6]:
        load.wait()
    pl.semaphore_wait(barrier, n_img + n_proj - 2)

    small = []
    moves = []
    for k, peer in enumerate(img_peers):
        for t, (ref, dst) in enumerate(((focus_ref, focus_all), (limit_ref, limit_all))):
            small.append(pltpu.make_async_remote_copy(
                src_ref=ref, dst_ref=dst.at[me], send_sem=small_send.at[t, k],
                recv_sem=small_recv.at[t, k], device_id={"img": peer}, device_id_type=MESH))
    for k, peer in enumerate(img_peers):
        moves.append(pltpu.make_async_remote_copy(
            src_ref=img.at[:, pl.ds(pl.multiple_of(peer * part, LANES), part)],
            dst_ref=moved.at[me], send_sem=img_send.at[k], recv_sem=img_recv.at[k],
            device_id={"img": peer}, device_id_type=MESH))
    for copy in small + moves:
        copy.start()

    def terms_chunk(c, carry):
        sin_v, cos_v = carry
        cols = pl.ds(pl.multiple_of(c * LANES, LANES), LANES)
        term = lane + (c * LANES).astype(jnp.float32)
        kept = jnp.where(term < limit, sin_v, 0.0)
        noisy = kept * noise_ref[:, cols]
        weighted[:, cols] = (noisy * img[:, cols].astype(jnp.float32)).astype(jnp.bfloat16)
        weighted_sq[:, cols] = (noisy * (-0.5 * sin_v)).astype(jnp.bfloat16)
        return sin_v * cos_d + cos_v * sin_d, cos_v * cos_d - sin_v * sin_d

    lax.fori_loop(0, width // LANES, terms_chunk, (sin0, cos0), unroll=2)
    loads[6].wait()

    depth = 512
    contract = (((1,), (1,)), ((), ()))

    def score_chunk(c, total):
        cols = pl.ds(pl.multiple_of(c * depth, depth), depth)
        rows = proj[:, cols]
        total = total + lax.dot_general(rows, weighted[:, cols], contract, preferred_element_type=jnp.float32)
        return total + lax.dot_general(rows * rows, weighted_sq[:, cols], contract,
                                       preferred_element_type=jnp.float32)

    scores = lax.fori_loop(0, width // depth, score_chunk, jnp.zeros((proj_rows, img_rows), jnp.float32))

    orient = lax.broadcasted_iota(jnp.int32, (proj_rows, img_rows), 0) + mine * proj_rows
    significant = orient < count_ref[...]
    peak = jnp.max(jnp.where(significant, scores, -1e30), axis=0, keepdims=True)
    expo = jnp.where(significant, jnp.exp(jnp.where(significant, scores - peak, 0.0)), 0.0)
    mass = jnp.sum(expo, axis=0, keepdims=True)
    stats[0:1, :] = peak
    stats[1:2, :] = mass
    terms[...] = expo.astype(jnp.bfloat16)

    stat_copies = []
    for k, peer in enumerate(proj_peers):
        stat_copies.append(pltpu.make_async_remote_copy(
            src_ref=stats, dst_ref=every_stats.at[mine], send_sem=stat_send.at[k],
            recv_sem=stat_recv.at[k], device_id={"proj": peer}, device_id_type=MESH))
        stat_copies[-1].start()
    post_copies = []
    for k, peer in enumerate(img_peers):
        post_copies.append(pltpu.make_async_remote_copy(
            src_ref=terms, dst_ref=every_terms.at[me], send_sem=post_send.at[k],
            recv_sem=post_recv.at[k], device_id={"img": peer}, device_id_type=MESH))
        post_copies[-1].start()

    for copy in small:
        copy.wait()
    focus_all[me] = focus_ref[...]
    limit_all[me] = limit_ref[...]
    start = (me * part).astype(jnp.float32)
    term0 = lane + start

    def weights_block(b, carry):
        focus_b = columns_of(focus_all[b], img_rows)
        limit_b = columns_of(limit_all[b].astype(jnp.float32), img_rows)
        sin_v, cos_v = sincos_turns(focus_b * ((term0 + 1.0) / width) + phase)
        sin_b, cos_b = sincos_turns(focus_b * (LANES / width))
        rows = pl.ds(pl.multiple_of(b * img_rows, img_rows), img_rows)
        for c in range(part // LANES):
            cols = slice(c * LANES, (c + 1) * LANES)
            kept = jnp.where(term0 + float(c * LANES) < limit_b, sin_v, 0.0)
            contrast[rows, cols] = kept
            back_wgt[rows, cols] = (kept * sin_v).astype(jnp.bfloat16)
            sin_v, cos_v = sin_v * cos_b + cos_v * sin_b, cos_v * cos_b - sin_v * sin_b
        return carry

    lax.fori_loop(0, n_img, weights_block, 0)

    every_stats[mine] = stats[...]
    for copy in stat_copies:
        copy.wait()
    peaks = [every_stats[q, 0:1, :] for q in range(n_proj)]
    top = functools.reduce(jnp.maximum, peaks)
    whole = sum(every_stats[q, 1:2, :] * jnp.exp(peaks[q] - top) for q in range(n_proj))
    evidence = top + jnp.log(whole)
    scale_out[0:1, :] = jnp.exp(peak - evidence)
    scale_out[1:2, :] = evidence
    scale_copies = []
    for k, peer in enumerate(img_peers):
        scale_copies.append(pltpu.make_async_remote_copy(
            src_ref=scale_out, dst_ref=every_scale.at[me], send_sem=scale_send.at[k],
            recv_sem=scale_recv.at[k], device_id={"img": peer}, device_id_type=MESH))
        scale_copies[-1].start()
    every_scale[me] = scale_out[...]

    def take_images(b, pixels):
        rows = pl.ds(pl.multiple_of(b * img_rows, img_rows), img_rows)
        back_img[rows, :] = (contrast[rows, :] * pixels.astype(jnp.float32)).astype(jnp.bfloat16)

    def take_post(b, values):
        cols = pl.ds(pl.multiple_of(b * img_rows, img_rows), img_rows)
        every_post[:, cols] = (values.astype(jnp.float32) * every_scale[b][0:1, :]).astype(jnp.bfloat16)

    take_images(me, img[:, pl.ds(pl.multiple_of(me * part, LANES), part)])
    every_post[:, pl.ds(pl.multiple_of(me * img_rows, img_rows), img_rows)] = (
        expo * every_scale[me][0:1, :]).astype(jnp.bfloat16)
    for k, source in enumerate(img_from):
        moves[k].wait()
        take_images(source, moved[source])
    for k, source in enumerate(img_from):
        post_copies[k].wait()
        scale_copies[k].wait()
        take_post(source, every_terms[source])

    step = min(part, 256)
    posts = every_post[...]
    for c in range(part // step):
        cols = slice(c * step, (c + 1) * step)
        sums = jnp.dot(posts, back_img[:, cols], preferred_element_type=jnp.float32)
        weights = jnp.dot(posts, back_wgt[:, cols], preferred_element_type=jnp.float32)
        rec_ref[:, cols] = (sums / (weights + 1.0)).astype(jnp.bfloat16)

    groups = img_rows // BLOCK
    group = lax.broadcasted_iota(jnp.int32, (1, img_rows), 1) // BLOCK
    placed = jnp.zeros((1, img_rows), jnp.float32)
    for a in range(n_img):
        plan = jnp.zeros((1, img_rows), jnp.int32)
        for g in range(groups):
            plan = jnp.where(group == g, plan_ref[a * groups + g], plan)
        values = every_scale[a][1:2, :]
        for t in range(groups):
            turned, target = values, plan
            if t:
                turned = pltpu.roll(values, t * BLOCK, 1)
                target = pltpu.roll(plan, t * BLOCK, 1)
            placed = placed + jnp.where(target == me * groups + group, turned, 0.0)
    ev_ref[...] = placed


def shards(n_img, n_proj, images, projections, noise_weight, defocus, orient_count, term_limit, block_plan):
    img_rows, width = images.shape
    proj_rows = projections.shape[0]
    part = width // n_img
    vmem = pl.BlockSpec(memory_space=pltpu.VMEM)
    hbm = pl.BlockSpec(memory_space=pl.ANY)
    bf16, f32 = jnp.bfloat16, jnp.float32
    dma = pltpu.SemaphoreType.DMA
    reconstruction, evidence = pl.pallas_call(
        functools.partial(kernel, n_img, n_proj),
        out_shape=(jax.ShapeDtypeStruct((proj_rows, part), bf16), jax.ShapeDtypeStruct((1, img_rows), f32)),
        in_specs=[hbm] * 7,
        out_specs=(vmem, vmem),
        scratch_shapes=[
            pltpu.VMEM((img_rows, width), bf16),
            pltpu.VMEM((proj_rows, width), bf16),
            pltpu.VMEM((1, width), f32),
            pltpu.VMEM((1, img_rows), f32),
            pltpu.VMEM((1, img_rows), jnp.int32),
            pltpu.VMEM((1, img_rows), jnp.int32),
            pltpu.SMEM(block_plan.shape, jnp.int32),
            pltpu.VMEM((img_rows, width), bf16),
            pltpu.VMEM((img_rows, width), bf16),
            pltpu.VMEM((n_img, img_rows, part), bf16),
            pltpu.VMEM((n_img * img_rows, part), f32),
            pltpu.VMEM((n_img * img_rows, part), bf16),
            pltpu.VMEM((n_img * img_rows, part), bf16),
            pltpu.VMEM((proj_rows, n_img * img_rows), bf16),
            pltpu.VMEM((n_img, 1, img_rows), f32),
            pltpu.VMEM((n_img, 1, img_rows), jnp.int32),
            pltpu.VMEM((proj_rows, img_rows), bf16),
            pltpu.VMEM((n_img, proj_rows, img_rows), bf16),
            pltpu.VMEM((2, img_rows), f32),
            pltpu.VMEM((n_proj, 2, img_rows), f32),
            pltpu.VMEM((2, img_rows), f32),
            pltpu.VMEM((n_img, 2, img_rows), f32),
            dma((7,)),
            dma((2, n_img)), dma((2, n_img)),
            dma((n_img,)), dma((n_img,)),
            dma((n_img,)), dma((n_img,)),
            dma((n_proj,)), dma((n_proj,)),
            dma((n_img,)), dma((n_img,)),
        ],
        compiler_params=pltpu.CompilerParams(
            collective_id=0, has_side_effects=True, vmem_limit_bytes=62 * 1024 * 1024),
    )(images, projections, noise_weight.reshape(1, -1), defocus.reshape(1, -1), orient_count.reshape(1, -1),
      term_limit.reshape(1, -1), block_plan)
    return reconstruction, evidence.reshape(-1)


def solution(mesh):
    n_img, n_proj = mesh.shape["img"], mesh.shape["proj"]
    placed = (P("img", None), P("proj", None), P(), P("img"), P("img"), P("img"), P())
    return jax.shard_map(
        functools.partial(shards, n_img, n_proj), mesh=mesh, in_specs=placed,
        out_specs=(P("proj", "img"), P("img")), check_vma=False,
    )
```

```python
import functools
import math

import jax
import jax.numpy as jnp
from jax import lax
from jax.experimental import pallas as pl
from jax.experimental.pallas import tpu as pltpu
from jax.sharding import PartitionSpec as P

BLOCK = 32
PIECES = 2
LANES = 128
MESH = pl.DeviceIdType.MESH
SIN_TERMS = [(-1.0) ** k * math.pi ** (2 * k + 1) / math.factorial(2 * k + 1) for k in range(7)]
COS_TERMS = [(-1.0) ** k * math.pi ** (2 * k) / math.factorial(2 * k) for k in range(8)]


def horner(terms, x):
    total = jnp.full_like(x, terms[-1])
    for term in terms[-2::-1]:
        total = total * x + term
    return total


def sincos_turns(turns):
    rest = turns - jnp.floor(turns + 0.5)
    square = rest * rest
    half_sin = rest * horner(SIN_TERMS, square)
    half_cos = horner(COS_TERMS, square)
    return 2.0 * half_sin * half_cos, 1.0 - 2.0 * half_sin * half_sin


def columns_of(row, rows):
    return jnp.broadcast_to(row, (LANES, rows)).T


def kernel(n_img, n_proj, img_hbm, proj_hbm, noise_hbm, focus_hbm, count_hbm, limit_hbm, plan_hbm,
           rec_ref, ev_ref,
           img, proj, noise_ref, focus_ref, count_ref, limit_ref, plan_ref, weighted, weighted_sq, moved, contrast, back_img, back_wgt, every_post,
           focus_all, limit_all, terms, every_terms, stats, every_stats, scale_out, every_scale,
           load_sem, small_send, small_recv, img_send, img_recv, pass_send, pass_recv, post_send, post_recv,
           stat_send, stat_recv, scale_send, scale_recv):
    me = lax.axis_index("img")
    mine = lax.axis_index("proj")
    img_rows, width = img.shape
    proj_rows = proj.shape[0]
    part = width // n_img
    chips = n_img // 2
    row_y, core = me // 2, lax.rem(me, 2)
    offsets = [(dy, dc) for dy in range(chips - 1, -1, -1) for dc in range(2) if dy or dc]
    img_peers = [lax.rem(row_y + dy, chips) * 2 + lax.rem(core + dc, 2) for dy, dc in offsets]
    img_from = [lax.rem(row_y + chips - dy, chips) * 2 + lax.rem(core + dc, 2) for dy, dc in offsets]
    side = lax.rem(mine, 2)
    beside = mine + 1 - 2 * side
    piece = img_rows // 2 // PIECES
    proj_peers = [lax.rem(mine + k, n_proj) for k in range(1, n_proj)]

    barrier = pltpu.get_barrier_semaphore()
    for peer in img_peers:
        pl.semaphore_signal(barrier, inc=1, device_id={"img": peer}, device_id_type=MESH)
    for peer in proj_peers:
        pl.semaphore_signal(barrier, inc=1, device_id={"proj": peer}, device_id_type=MESH)
    sources = (focus_hbm, limit_hbm, img_hbm, noise_hbm, count_hbm, plan_hbm, proj_hbm)
    targets = (focus_ref, limit_ref, img, noise_ref, count_ref, plan_ref, proj)
    loads = [pltpu.make_async_copy(source, target, load_sem.at[n])
             for n, (source, target) in enumerate(zip(sources, targets))]
    for load in loads:
        load.start()
    loads[0].wait()
    loads[1].wait()

    lane = lax.broadcasted_iota(jnp.int32, (1, LANES), 1).astype(jnp.float32)
    phase = 0.1 / (2.0 * math.pi)
    focus = columns_of(focus_ref[...], img_rows)
    limit = columns_of(limit_ref[...].astype(jnp.float32), img_rows)
    sin0, cos0 = sincos_turns(focus * ((lane + 1.0) / width) + phase)
    sin_d, cos_d = sincos_turns(focus * (LANES / width))

    for load in loads[2:6]:
        load.wait()

    def terms_chunk(c, carry):
        sin_v, cos_v = carry
        cols = pl.ds(pl.multiple_of(c * LANES, LANES), LANES)
        term = lane + (c * LANES).astype(jnp.float32)
        kept = jnp.where(term < limit, sin_v, 0.0)
        noisy = kept * noise_ref[:, cols]
        weighted[:, cols] = (noisy * img[:, cols].astype(jnp.float32)).astype(jnp.bfloat16)
        weighted_sq[:, cols] = (noisy * (-0.5 * sin_v)).astype(jnp.bfloat16)
        return sin_v * cos_d + cos_v * sin_d, cos_v * cos_d - sin_v * sin_d

    lax.fori_loop(0, width // LANES, terms_chunk, (sin0, cos0), unroll=2)
    loads[6].wait()

    depth = 512
    contract = (((1,), (1,)), ((), ()))

    def score_chunk(c, total):
        cols = pl.ds(pl.multiple_of(c * depth, depth), depth)
        rows = proj[:, cols]
        total = total + lax.dot_general(rows, weighted[:, cols], contract, preferred_element_type=jnp.float32)
        return total + lax.dot_general(rows * rows, weighted_sq[:, cols], contract,
                                       preferred_element_type=jnp.float32)

    scores = lax.fori_loop(0, width // depth, score_chunk, jnp.zeros((proj_rows, img_rows), jnp.float32))

    orient = lax.broadcasted_iota(jnp.int32, (proj_rows, img_rows), 0) + mine * proj_rows
    significant = orient < count_ref[...]
    peak = jnp.max(jnp.where(significant, scores, -1e30), axis=0, keepdims=True)
    expo = jnp.where(significant, jnp.exp(jnp.where(significant, scores - peak, 0.0)), 0.0)
    mass = jnp.sum(expo, axis=0, keepdims=True)
    stats[0:1, :] = peak
    stats[1:2, :] = mass
    terms[...] = expo.astype(jnp.bfloat16)

    pl.semaphore_wait(barrier, n_img + n_proj - 2)

    small = []
    for k, peer in enumerate(img_peers):
        for t, (ref, dst) in enumerate(((focus_ref, focus_all), (limit_ref, limit_all))):
            small.append(pltpu.make_async_remote_copy(
                src_ref=ref, dst_ref=dst.at[me], send_sem=small_send.at[t, k],
                recv_sem=small_recv.at[t, k], device_id={"img": peer}, device_id_type=MESH))
            small[-1].start()
    stat_copies = []
    for k, peer in enumerate(proj_peers):
        stat_copies.append(pltpu.make_async_remote_copy(
            src_ref=stats, dst_ref=every_stats.at[mine], send_sem=stat_send.at[k],
            recv_sem=stat_recv.at[k], device_id={"proj": peer}, device_id_type=MESH))
        stat_copies[-1].start()
    moves = []
    for k, peer in enumerate(img_peers):
        slab = pl.ds(pl.multiple_of(peer * part, LANES), part)
        if offsets[k][0]:
            for n in range(PIECES):
                rows = pl.ds(pl.multiple_of((side * PIECES + n) * piece, piece), piece)
                moves.append((k, n, pltpu.make_async_remote_copy(
                    src_ref=img.at[rows, slab], dst_ref=moved.at[me, rows, :], send_sem=img_send.at[k, n],
                    recv_sem=img_recv.at[k, n], device_id={"img": peer}, device_id_type=MESH)))
        else:
            near = pltpu.make_async_remote_copy(
                src_ref=img.at[:, slab], dst_ref=moved.at[me], send_sem=img_send.at[k, 0],
                recv_sem=img_recv.at[k, 0], device_id={"img": peer}, device_id_type=MESH)
    for _, _, copy in moves:
        copy.start()
    near.start()
    post_copies = []
    for k, peer in enumerate(img_peers):
        post_copies.append(pltpu.make_async_remote_copy(
            src_ref=terms, dst_ref=every_terms.at[me], send_sem=post_send.at[k],
            recv_sem=post_recv.at[k], device_id={"img": peer}, device_id_type=MESH))
        post_copies[-1].start()

    for copy in small:
        copy.wait()
    focus_all[me] = focus_ref[...]
    limit_all[me] = limit_ref[...]
    start = (me * part).astype(jnp.float32)
    term0 = lane + start

    def weights_block(b, carry):
        focus_b = columns_of(focus_all[b], img_rows)
        limit_b = columns_of(limit_all[b].astype(jnp.float32), img_rows)
        sin_v, cos_v = sincos_turns(focus_b * ((term0 + 1.0) / width) + phase)
        sin_b, cos_b = sincos_turns(focus_b * (LANES / width))
        rows = pl.ds(pl.multiple_of(b * img_rows, img_rows), img_rows)
        for c in range(part // LANES):
            cols = slice(c * LANES, (c + 1) * LANES)
            kept = jnp.where(term0 + float(c * LANES) < limit_b, sin_v, 0.0)
            contrast[rows, cols] = kept
            back_wgt[rows, cols] = (kept * sin_v).astype(jnp.bfloat16)
            sin_v, cos_v = sin_v * cos_b + cos_v * sin_b, cos_v * cos_b - sin_v * sin_b
        return carry

    lax.fori_loop(0, n_img, weights_block, 0)

    every_stats[mine] = stats[...]
    for copy in stat_copies:
        copy.wait()
    peaks = [every_stats[q, 0:1, :] for q in range(n_proj)]
    top = functools.reduce(jnp.maximum, peaks)
    whole = sum(every_stats[q, 1:2, :] * jnp.exp(peaks[q] - top) for q in range(n_proj))
    evidence = top + jnp.log(whole)
    scale_out[0:1, :] = jnp.exp(peak - evidence)
    scale_out[1:2, :] = evidence
    scale_copies = []
    for k, peer in enumerate(img_peers):
        scale_copies.append(pltpu.make_async_remote_copy(
            src_ref=scale_out, dst_ref=every_scale.at[me], send_sem=scale_send.at[k],
            recv_sem=scale_recv.at[k], device_id={"img": peer}, device_id_type=MESH))
        scale_copies[-1].start()
    every_scale[me] = scale_out[...]

    def take_images(b, pixels):
        rows = pl.ds(pl.multiple_of(b * img_rows, img_rows), img_rows)
        back_img[rows, :] = (contrast[rows, :] * pixels.astype(jnp.float32)).astype(jnp.bfloat16)

    def take_post(b, values):
        cols = pl.ds(pl.multiple_of(b * img_rows, img_rows), img_rows)
        every_post[:, cols] = (values.astype(jnp.float32) * every_scale[b][0:1, :]).astype(jnp.bfloat16)

    take_images(me, img[:, pl.ds(pl.multiple_of(me * part, LANES), part)])
    every_post[:, pl.ds(pl.multiple_of(me * img_rows, img_rows), img_rows)] = (
        expo * every_scale[me][0:1, :]).astype(jnp.bfloat16)
    near.wait()
    take_images(img_from[-1], moved[img_from[-1]])
    passed = []
    for k, n, copy in moves:
        copy.wait()
        held = moved.at[img_from[k], pl.ds(pl.multiple_of((side * PIECES + n) * piece, piece), piece), :]
        passed.append(pltpu.make_async_remote_copy(
            src_ref=held, dst_ref=held, send_sem=pass_send.at[k, n], recv_sem=pass_recv.at[k, n],
            device_id={"proj": beside}, device_id_type=MESH))
        passed[-1].start()
    for k, source in enumerate(img_from):
        post_copies[k].wait()
        scale_copies[k].wait()
        take_post(source, every_terms[source])
    for copy in passed:
        copy.wait()
    for source in img_from[:-1]:
        take_images(source, moved[source])

    step = min(part, 256)
    posts = every_post[...]
    for c in range(part // step):
        cols = slice(c * step, (c + 1) * step)
        sums = jnp.dot(posts, back_img[:, cols], preferred_element_type=jnp.float32)
        weights = jnp.dot(posts, back_wgt[:, cols], preferred_element_type=jnp.float32)
        rec_ref[:, cols] = (sums / (weights + 1.0)).astype(jnp.bfloat16)

    groups = img_rows // BLOCK
    group = lax.broadcasted_iota(jnp.int32, (1, img_rows), 1) // BLOCK
    placed = jnp.zeros((1, img_rows), jnp.float32)
    for a in range(n_img):
        plan = jnp.zeros((1, img_rows), jnp.int32)
        for g in range(groups):
            plan = jnp.where(group == g, plan_ref[a * groups + g], plan)
        values = every_scale[a][1:2, :]
        for t in range(groups):
            turned, target = values, plan
            if t:
                turned = pltpu.roll(values, t * BLOCK, 1)
                target = pltpu.roll(plan, t * BLOCK, 1)
            placed = placed + jnp.where(target == me * groups + group, turned, 0.0)
    ev_ref[...] = placed


def shards(n_img, n_proj, images, projections, noise_weight, defocus, orient_count, term_limit, block_plan):
    img_rows, width = images.shape
    proj_rows = projections.shape[0]
    part = width // n_img
    vmem = pl.BlockSpec(memory_space=pltpu.VMEM)
    hbm = pl.BlockSpec(memory_space=pl.ANY)
    bf16, f32 = jnp.bfloat16, jnp.float32
    dma = pltpu.SemaphoreType.DMA
    reconstruction, evidence = pl.pallas_call(
        functools.partial(kernel, n_img, n_proj),
        out_shape=(jax.ShapeDtypeStruct((proj_rows, part), bf16), jax.ShapeDtypeStruct((1, img_rows), f32)),
        in_specs=[hbm] * 7,
        out_specs=(vmem, vmem),
        scratch_shapes=[
            pltpu.VMEM((img_rows, width), bf16),
            pltpu.VMEM((proj_rows, width), bf16),
            pltpu.VMEM((1, width), f32),
            pltpu.VMEM((1, img_rows), f32),
            pltpu.VMEM((1, img_rows), jnp.int32),
            pltpu.VMEM((1, img_rows), jnp.int32),
            pltpu.SMEM(block_plan.shape, jnp.int32),
            pltpu.VMEM((img_rows, width), bf16),
            pltpu.VMEM((img_rows, width), bf16),
            pltpu.VMEM((n_img, img_rows, part), bf16),
            pltpu.VMEM((n_img * img_rows, part), f32),
            pltpu.VMEM((n_img * img_rows, part), bf16),
            pltpu.VMEM((n_img * img_rows, part), bf16),
            pltpu.VMEM((proj_rows, n_img * img_rows), bf16),
            pltpu.VMEM((n_img, 1, img_rows), f32),
            pltpu.VMEM((n_img, 1, img_rows), jnp.int32),
            pltpu.VMEM((proj_rows, img_rows), bf16),
            pltpu.VMEM((n_img, proj_rows, img_rows), bf16),
            pltpu.VMEM((2, img_rows), f32),
            pltpu.VMEM((n_proj, 2, img_rows), f32),
            pltpu.VMEM((2, img_rows), f32),
            pltpu.VMEM((n_img, 2, img_rows), f32),
            dma((7,)),
            dma((2, n_img)), dma((2, n_img)),
            dma((n_img, PIECES)), dma((n_img, PIECES)),
            dma((n_img, PIECES)), dma((n_img, PIECES)),
            dma((n_img,)), dma((n_img,)),
            dma((n_proj,)), dma((n_proj,)),
            dma((n_img,)), dma((n_img,)),
        ],
        compiler_params=pltpu.CompilerParams(
            collective_id=0, has_side_effects=True, vmem_limit_bytes=62 * 1024 * 1024),
    )(images, projections, noise_weight.reshape(1, -1), defocus.reshape(1, -1), orient_count.reshape(1, -1),
      term_limit.reshape(1, -1), block_plan)
    return reconstruction, evidence.reshape(-1)


def solution(mesh):
    n_img, n_proj = mesh.shape["img"], mesh.shape["proj"]
    placed = (P("img", None), P("proj", None), P(), P("img"), P("img"), P("img"), P())
    return jax.shard_map(
        functools.partial(shards, n_img, n_proj), mesh=mesh, in_specs=placed,
        out_specs=(P("proj", "img"), P("img")), check_vma=False,
    )
```

```python
import functools
import math

import jax
import jax.numpy as jnp
from jax import lax
from jax.experimental import pallas as pl
from jax.experimental.pallas import tpu as pltpu
from jax.sharding import PartitionSpec as P

BLOCK = 32
PIECES = 2
LANES = 128
MESH = pl.DeviceIdType.MESH
SIN_TERMS = [(-1.0) ** k * math.pi ** (2 * k + 1) / math.factorial(2 * k + 1) for k in range(7)]
COS_TERMS = [(-1.0) ** k * math.pi ** (2 * k) / math.factorial(2 * k) for k in range(8)]


def horner(terms, x):
    total = jnp.full_like(x, terms[-1])
    for term in terms[-2::-1]:
        total = total * x + term
    return total


def sincos_turns(turns):
    rest = turns - jnp.floor(turns + 0.5)
    square = rest * rest
    half_sin = rest * horner(SIN_TERMS, square)
    half_cos = horner(COS_TERMS, square)
    return 2.0 * half_sin * half_cos, 1.0 - 2.0 * half_sin * half_sin


def columns_of(row, rows):
    return jnp.broadcast_to(row, (LANES, rows)).T


def kernel(n_img, n_proj, img_hbm, proj_hbm, noise_hbm, focus_hbm, count_hbm, limit_hbm, plan_hbm,
           rec_ref, ev_ref,
           img, proj, noise_ref, focus_ref, count_ref, limit_ref, plan_ref, weighted, weighted_sq, moved, contrast, back_img, back_wgt, every_post,
           focus_all, limit_all, terms, every_terms, stats, every_stats, scale_out, every_scale,
           load_sem, small_send, small_recv, img_send, img_recv, pass_send, pass_recv, post_send, post_recv,
           stat_send, stat_recv, scale_send, scale_recv):
    me = lax.axis_index("img")
    mine = lax.axis_index("proj")
    img_rows, width = img.shape
    proj_rows = proj.shape[0]
    part = width // n_img
    chips = n_img // 2
    row_y, core = me // 2, lax.rem(me, 2)
    offsets = [(dy, dc) for dy in range(chips - 1, -1, -1) for dc in range(2) if dy or dc]
    img_peers = [lax.rem(row_y + dy, chips) * 2 + lax.rem(core + dc, 2) for dy, dc in offsets]
    img_from = [lax.rem(row_y + chips - dy, chips) * 2 + lax.rem(core + dc, 2) for dy, dc in offsets]
    side = lax.rem(mine, 2)
    beside = mine + 1 - 2 * side
    piece = img_rows // 2 // PIECES
    proj_peers = [lax.rem(mine + k, n_proj) for k in range(1, n_proj)]

    barrier = pltpu.get_barrier_semaphore()
    for peer in img_peers:
        pl.semaphore_signal(barrier, inc=1, device_id={"img": peer}, device_id_type=MESH)
    for peer in proj_peers:
        pl.semaphore_signal(barrier, inc=1, device_id={"proj": peer}, device_id_type=MESH)
    sources = (focus_hbm, limit_hbm, img_hbm, noise_hbm, count_hbm, plan_hbm, proj_hbm)
    targets = (focus_ref, limit_ref, img, noise_ref, count_ref, plan_ref, proj)
    loads = [pltpu.make_async_copy(source, target, load_sem.at[n])
             for n, (source, target) in enumerate(zip(sources, targets))]
    for load in loads:
        load.start()
    loads[0].wait()
    loads[1].wait()

    lane = lax.broadcasted_iota(jnp.int32, (1, LANES), 1).astype(jnp.float32)
    phase = 0.1 / (2.0 * math.pi)
    focus = columns_of(focus_ref[...], img_rows)
    limit = columns_of(limit_ref[...].astype(jnp.float32), img_rows)
    sin0, cos0 = sincos_turns(focus * ((lane + 1.0) / width) + phase)
    sin_d, cos_d = sincos_turns(focus * (LANES / width))

    for load in loads[2:6]:
        load.wait()

    def terms_chunk(c, carry):
        sin_v, cos_v = carry
        cols = pl.ds(pl.multiple_of(c * LANES, LANES), LANES)
        term = lane + (c * LANES).astype(jnp.float32)
        kept = jnp.where(term < limit, sin_v, 0.0)
        noisy = kept * noise_ref[:, cols]
        weighted[:, cols] = (noisy * img[:, cols].astype(jnp.float32)).astype(jnp.bfloat16)
        weighted_sq[:, cols] = (noisy * (-0.5 * sin_v)).astype(jnp.bfloat16)
        return sin_v * cos_d + cos_v * sin_d, cos_v * cos_d - sin_v * sin_d

    lax.fori_loop(0, width // LANES, terms_chunk, (sin0, cos0), unroll=2)
    loads[6].wait()

    depth = 512
    contract = (((1,), (1,)), ((), ()))

    def score_chunk(c, total):
        cols = pl.ds(pl.multiple_of(c * depth, depth), depth)
        rows = proj[:, cols]
        total = total + lax.dot_general(rows, weighted[:, cols], contract, preferred_element_type=jnp.float32)
        return total + lax.dot_general(rows * rows, weighted_sq[:, cols], contract,
                                       preferred_element_type=jnp.float32)

    scores = lax.fori_loop(0, width // depth, score_chunk, jnp.zeros((proj_rows, img_rows), jnp.float32))

    orient = lax.broadcasted_iota(jnp.int32, (proj_rows, img_rows), 0) + mine * proj_rows
    significant = orient < count_ref[...]
    peak = jnp.max(jnp.where(significant, scores, -1e30), axis=0, keepdims=True)
    expo = jnp.where(significant, jnp.exp(jnp.where(significant, scores - peak, 0.0)), 0.0)
    mass = jnp.sum(expo, axis=0, keepdims=True)
    stats[0:1, :] = peak
    stats[1:2, :] = mass
    terms[...] = expo.astype(jnp.bfloat16)

    pl.semaphore_wait(barrier, n_img + n_proj - 2)

    small = []
    for k, peer in enumerate(img_peers):
        for t, (ref, dst) in enumerate(((focus_ref, focus_all), (limit_ref, limit_all))):
            small.append(pltpu.make_async_remote_copy(
                src_ref=ref, dst_ref=dst.at[me], send_sem=small_send.at[t, k],
                recv_sem=small_recv.at[t, k], device_id={"img": peer}, device_id_type=MESH))
            small[-1].start()
    stat_copies = []
    for k, peer in enumerate(proj_peers):
        stat_copies.append(pltpu.make_async_remote_copy(
            src_ref=stats, dst_ref=every_stats.at[mine], send_sem=stat_send.at[k],
            recv_sem=stat_recv.at[k], device_id={"proj": peer}, device_id_type=MESH))
        stat_copies[-1].start()
    moves = []
    for k, peer in enumerate(img_peers):
        slab = pl.ds(pl.multiple_of(peer * part, LANES), part)
        if offsets[k][0]:
            for n in range(PIECES):
                rows = pl.ds(pl.multiple_of((side * PIECES + n) * piece, piece), piece)
                moves.append((k, n, pltpu.make_async_remote_copy(
                    src_ref=img.at[rows, slab], dst_ref=moved.at[me, rows, :], send_sem=img_send.at[k, n],
                    recv_sem=img_recv.at[k, n], device_id={"img": peer}, device_id_type=MESH)))
        else:
            near = pltpu.make_async_remote_copy(
                src_ref=img.at[:, slab], dst_ref=moved.at[me], send_sem=img_send.at[k, 0],
                recv_sem=img_recv.at[k, 0], device_id={"img": peer}, device_id_type=MESH)
    for _, _, copy in moves:
        copy.start()
    near.start()
    post_copies = []
    for k, peer in enumerate(img_peers):
        post_copies.append(pltpu.make_async_remote_copy(
            src_ref=terms, dst_ref=every_terms.at[me], send_sem=post_send.at[k],
            recv_sem=post_recv.at[k], device_id={"img": peer}, device_id_type=MESH))
        if offsets[k] == (0, 1) or not offsets[k][1]:
            post_copies[-1].start()

    for copy in small:
        copy.wait()
    focus_all[me] = focus_ref[...]
    limit_all[me] = limit_ref[...]
    start = (me * part).astype(jnp.float32)
    term0 = lane + start

    def weights_block(b, carry):
        focus_b = columns_of(focus_all[b], img_rows)
        limit_b = columns_of(limit_all[b].astype(jnp.float32), img_rows)
        sin_v, cos_v = sincos_turns(focus_b * ((term0 + 1.0) / width) + phase)
        sin_b, cos_b = sincos_turns(focus_b * (LANES / width))
        rows = pl.ds(pl.multiple_of(b * img_rows, img_rows), img_rows)
        for c in range(part // LANES):
            cols = slice(c * LANES, (c + 1) * LANES)
            kept = jnp.where(term0 + float(c * LANES) < limit_b, sin_v, 0.0)
            contrast[rows, cols] = kept
            back_wgt[rows, cols] = (kept * sin_v).astype(jnp.bfloat16)
            sin_v, cos_v = sin_v * cos_b + cos_v * sin_b, cos_v * cos_b - sin_v * sin_b
        return carry

    lax.fori_loop(0, n_img, weights_block, 0)

    every_stats[mine] = stats[...]
    for copy in stat_copies:
        copy.wait()
    peaks = [every_stats[q, 0:1, :] for q in range(n_proj)]
    top = functools.reduce(jnp.maximum, peaks)
    whole = sum(every_stats[q, 1:2, :] * jnp.exp(peaks[q] - top) for q in range(n_proj))
    evidence = top + jnp.log(whole)
    scale_out[0:1, :] = jnp.exp(peak - evidence)
    scale_out[1:2, :] = evidence
    scale_copies = []
    for k, peer in enumerate(img_peers):
        scale_copies.append(pltpu.make_async_remote_copy(
            src_ref=scale_out, dst_ref=every_scale.at[me], send_sem=scale_send.at[k],
            recv_sem=scale_recv.at[k], device_id={"img": peer}, device_id_type=MESH))
        scale_copies[-1].start()
    every_scale[me] = scale_out[...]

    def take_images(b, pixels):
        rows = pl.ds(pl.multiple_of(b * img_rows, img_rows), img_rows)
        back_img[rows, :] = (contrast[rows, :] * pixels.astype(jnp.float32)).astype(jnp.bfloat16)

    def take_post(b, values):
        cols = pl.ds(pl.multiple_of(b * img_rows, img_rows), img_rows)
        every_post[:, cols] = (values.astype(jnp.float32) * every_scale[b][0:1, :]).astype(jnp.bfloat16)

    take_images(me, img[:, pl.ds(pl.multiple_of(me * part, LANES), part)])
    every_post[:, pl.ds(pl.multiple_of(me * img_rows, img_rows), img_rows)] = (
        expo * every_scale[me][0:1, :]).astype(jnp.bfloat16)
    near.wait()
    take_images(img_from[-1], moved[img_from[-1]])
    passed = []
    for k, n, copy in moves:
        copy.wait()
        held = moved.at[img_from[k], pl.ds(pl.multiple_of((side * PIECES + n) * piece, piece), piece), :]
        passed.append(pltpu.make_async_remote_copy(
            src_ref=held, dst_ref=held, send_sem=pass_send.at[k, n], recv_sem=pass_recv.at[k, n],
            device_id={"proj": beside}, device_id_type=MESH))
        passed[-1].start()
    for k, source in enumerate(img_from):
        post_copies[k].wait()
        if not offsets[k][1]:
            held = every_terms.at[source]
            post_copies[k + 1] = pltpu.make_async_remote_copy(
                src_ref=held, dst_ref=held, send_sem=post_send.at[k + 1], recv_sem=post_recv.at[k + 1],
                device_id={"img": img_peers[-1]}, device_id_type=MESH)
            post_copies[k + 1].start()
        scale_copies[k].wait()
        take_post(source, every_terms[source])
    for copy in passed:
        copy.wait()
    for source in img_from[:-1]:
        take_images(source, moved[source])

    step = min(part, 256)
    posts = every_post[...]
    for c in range(part // step):
        cols = slice(c * step, (c + 1) * step)
        sums = jnp.dot(posts, back_img[:, cols], preferred_element_type=jnp.float32)
        weights = jnp.dot(posts, back_wgt[:, cols], preferred_element_type=jnp.float32)
        rec_ref[:, cols] = (sums / (weights + 1.0)).astype(jnp.bfloat16)

    groups = img_rows // BLOCK
    group = lax.broadcasted_iota(jnp.int32, (1, img_rows), 1) // BLOCK
    placed = jnp.zeros((1, img_rows), jnp.float32)
    for a in range(n_img):
        plan = jnp.zeros((1, img_rows), jnp.int32)
        for g in range(groups):
            plan = jnp.where(group == g, plan_ref[a * groups + g], plan)
        values = every_scale[a][1:2, :]
        for t in range(groups):
            turned, target = values, plan
            if t:
                turned = pltpu.roll(values, t * BLOCK, 1)
                target = pltpu.roll(plan, t * BLOCK, 1)
            placed = placed + jnp.where(target == me * groups + group, turned, 0.0)
    ev_ref[...] = placed


def shards(n_img, n_proj, images, projections, noise_weight, defocus, orient_count, term_limit, block_plan):
    img_rows, width = images.shape
    proj_rows = projections.shape[0]
    part = width // n_img
    vmem = pl.BlockSpec(memory_space=pltpu.VMEM)
    hbm = pl.BlockSpec(memory_space=pl.ANY)
    bf16, f32 = jnp.bfloat16, jnp.float32
    dma = pltpu.SemaphoreType.DMA
    reconstruction, evidence = pl.pallas_call(
        functools.partial(kernel, n_img, n_proj),
        out_shape=(jax.ShapeDtypeStruct((proj_rows, part), bf16), jax.ShapeDtypeStruct((1, img_rows), f32)),
        in_specs=[hbm] * 7,
        out_specs=(vmem, vmem),
        scratch_shapes=[
            pltpu.VMEM((img_rows, width), bf16),
            pltpu.VMEM((proj_rows, width), bf16),
            pltpu.VMEM((1, width), f32),
            pltpu.VMEM((1, img_rows), f32),
            pltpu.VMEM((1, img_rows), jnp.int32),
            pltpu.VMEM((1, img_rows), jnp.int32),
            pltpu.SMEM(block_plan.shape, jnp.int32),
            pltpu.VMEM((img_rows, width), bf16),
            pltpu.VMEM((img_rows, width), bf16),
            pltpu.VMEM((n_img, img_rows, part), bf16),
            pltpu.VMEM((n_img * img_rows, part), f32),
            pltpu.VMEM((n_img * img_rows, part), bf16),
            pltpu.VMEM((n_img * img_rows, part), bf16),
            pltpu.VMEM((proj_rows, n_img * img_rows), bf16),
            pltpu.VMEM((n_img, 1, img_rows), f32),
            pltpu.VMEM((n_img, 1, img_rows), jnp.int32),
            pltpu.VMEM((proj_rows, img_rows), bf16),
            pltpu.VMEM((n_img, proj_rows, img_rows), bf16),
            pltpu.VMEM((2, img_rows), f32),
            pltpu.VMEM((n_proj, 2, img_rows), f32),
            pltpu.VMEM((2, img_rows), f32),
            pltpu.VMEM((n_img, 2, img_rows), f32),
            dma((7,)),
            dma((2, n_img)), dma((2, n_img)),
            dma((n_img, PIECES)), dma((n_img, PIECES)),
            dma((n_img, PIECES)), dma((n_img, PIECES)),
            dma((n_img,)), dma((n_img,)),
            dma((n_proj,)), dma((n_proj,)),
            dma((n_img,)), dma((n_img,)),
        ],
        compiler_params=pltpu.CompilerParams(
            collective_id=0, has_side_effects=True, vmem_limit_bytes=62 * 1024 * 1024),
    )(images, projections, noise_weight.reshape(1, -1), defocus.reshape(1, -1), orient_count.reshape(1, -1),
      term_limit.reshape(1, -1), block_plan)
    return reconstruction, evidence.reshape(-1)


def solution(mesh):
    n_img, n_proj = mesh.shape["img"], mesh.shape["proj"]
    placed = (P("img", None), P("proj", None), P(), P("img"), P("img"), P("img"), P())
    return jax.shard_map(
        functools.partial(shards, n_img, n_proj), mesh=mesh, in_specs=placed,
        out_specs=(P("proj", "img"), P("img")), check_vma=False,
    )
```
